256 devices in a mesh: group: 2 (over y), seq: 128 (over x, z, core).
Axes of the slice: x: 4, y: 2, z: 16, core: 2. Of those that a mesh axis runs over, the one named last changes fastest.
The devices are a block of a 4x16x16 slice.
Arguments:
- query_frames: bfloat16 [131072, 4096], P(('group', 'seq')), parts along dimension 0, may hold values from -5 to 5
- key_frames: bfloat16 [131072, 512], P(('group', 'seq')), parts along dimension 0, may hold values from -5 to 5
- value_frames: bfloat16 [131072, 512], P(('group', 'seq')), parts along dimension 0, may hold values from -6 to 6
- token_counts: int32 [256], P(('group', 'seq')), parts along dimension 0, may hold values from 1 to 511, as said below
- segments: int32 [65536], P('group'), parts along dimension 0, may hold values from 0 to 63, as said below
Outputs:
- attended: bfloat16 [65536, 4096], P(('group', 'seq')), parts along dimension 0
The draws below stay inside these ranges and needn't reach their ends.
There are 2 independent parts, one for each index of `group`. The reference program is written for one: setup_inputs(seed, part) draws one part's arguments, and reference() takes and returns one part's arrays. A program takes and returns all parts, laid end to end along the dimension named above; each array names one. Nothing has to cross between parts.
Inputs may be any that keep to these rules, and one draw needn't show every extreme that they name: `token_counts`: entry d belongs to device d of seq. The counts before entry d sum to a number from d * 256 to d * 256 + 255, and all counts sum to 32768. `segments`: sequence numbers never fall along the positions and each of 0 to 63 appears; each packed sequence covers 1 to 1024 consecutive positions, one exactly 1024; the first covers more than 256.
All inputs are finite; a program needn't handle non-finite values.
Results may differ from the reference program's by a relative error of at most 0.013.
Values may be sent and summed in bfloat16 or wider, within the bound.
A program may use at most 64 MiB of HBM per device.

```python
import math
import jax
import jax.numpy as jnp
from jax import lax

Q_HEADS = 32
KV_HEADS = 4
HEAD_DIM = 128
SPAN = 256
WINDOW = 5
CYCLE = 128
FRAME_CAP = 512
FRAME_ROWS = 65536
SEQ_LEN = 32768
CLIPS = 64
QW = 4096
KW = 512


def draw_query_frames(key, part):
    groups = Q_HEADS // KV_HEADS
    shape = (FRAME_ROWS, KV_HEADS, groups, HEAD_DIM)
    values = jnp.clip(jax.random.normal(jax.random.fold_in(key, 1), shape, jnp.float32), -5.0, 5.0)
    return values.reshape(FRAME_ROWS, Q_HEADS * HEAD_DIM).astype(jnp.bfloat16)


def draw_key_frames(key, part):
    shape = (FRAME_ROWS, KV_HEADS, HEAD_DIM)
    values = jnp.clip(jax.random.normal(jax.random.fold_in(key, 2), shape, jnp.float32), -5.0, 5.0)
    return values.reshape(FRAME_ROWS, KV_HEADS * HEAD_DIM).astype(jnp.bfloat16)


def draw_token_counts(key, part):
    places = jnp.arange(CYCLE + 1, dtype=jnp.int32)
    leads = jax.random.randint(jax.random.fold_in(key, 21), (CYCLE + 1,), 0, SPAN, dtype=jnp.int32)
    widest = jax.random.randint(jax.random.fold_in(key, 22), (), 0, CYCLE - 1, dtype=jnp.int32)
    leads = jnp.where(places == widest, 0, leads)
    leads = jnp.where(places == widest + 1, SPAN - 1, leads)
    leads = jnp.where((places == 0) | (places == CYCLE), 0, leads)
    return (SPAN + leads[1:] - leads[:-1]).astype(jnp.int32)


def draw_segments(key, part):
    marks = jnp.arange(CLIPS + 1, dtype=jnp.int32)
    shifts = jax.random.randint(jax.random.fold_in(key, 31), (CLIPS + 1,), 1 - SPAN, SPAN, dtype=jnp.int32)
    firsts = jax.random.randint(jax.random.fold_in(key, 32), (), 0, SPAN, dtype=jnp.int32)
    shifts = jnp.where(marks == 1, firsts, shifts)
    widest = jax.random.randint(jax.random.fold_in(key, 33), (), 3, CLIPS, dtype=jnp.int32)
    shifts = jnp.where(marks == widest - 1, -SPAN, shifts)
    shifts = jnp.where(marks == widest, SPAN, shifts)
    shifts = jnp.where((marks == 0) | (marks == CLIPS), 0, shifts)
    bounds = (2 * SPAN * marks + shifts)[1:CLIPS]
    places = jnp.arange(SEQ_LEN, dtype=jnp.int32)
    return jnp.sum((places[:, None] >= bounds[None, :]).astype(jnp.int32), axis=1).astype(jnp.int32)


def block_levels(rng, dims, cuts, smallest, top_value):
    def one(position, parts):
        draws = jax.random.uniform(jax.random.fold_in(jax.random.fold_in(rng, 6), position), (parts,), jnp.float32, smallest / len(cuts), top_value / len(cuts))
        return jnp.repeat(jnp.exp(draws), dims[position] // parts).reshape((-1,) + (1,) * (len(dims) - position - 1))

    factor_of = one(*cuts[0])
    for cut in cuts[1:]:
        factor_of = factor_of * one(*cut)
    return factor_of


def normal_values(own_key, shape, width, bound, shards=(), kind=jnp.bfloat16):
    drawn = width * jax.random.normal(own_key, shape, jnp.float32)
    if shards:
        drawn = drawn * block_levels(own_key, shape, shards, -0.22, 0.18)
    return jnp.clip(drawn, -bound, bound).astype(kind)


def setup_inputs(seed: int = 0, part: int = 0) -> dict:
    streams_of = jax.random.split(jax.random.key(seed), 6)
    part_keys = jax.random.split(jax.random.fold_in(streams_of[5], part), 6)
    return {
        "query_frames": draw_query_frames(jax.random.fold_in(jax.random.fold_in(streams_of[5], part), 71), part),
        "key_frames": draw_key_frames(jax.random.fold_in(jax.random.fold_in(streams_of[5], part), 71), part),
        "value_frames": normal_values(part_keys[2], (FRAME_ROWS, KW), 1.0, 6.0, ((0, 128),)),
        "token_counts": draw_token_counts(jax.random.fold_in(jax.random.fold_in(streams_of[5], part), 71), part),
        "segments": draw_segments(jax.random.fold_in(jax.random.fold_in(streams_of[5], part), 71), part),
    }


def reference(query_frames, key_frames, value_frames, token_counts, segments):
    counts = token_counts.astype(jnp.int32)
    offsets = (jnp.cumsum(counts) - counts).astype(jnp.int32)
    places = jnp.arange(SEQ_LEN, dtype=jnp.int32)
    owners = (jnp.searchsorted(offsets, places, side='right') - 1).astype(jnp.int32)
    source = (owners * FRAME_CAP + places - offsets[owners]).astype(jnp.int32)
    queries = query_frames[source]
    keys = key_frames[source]
    values = value_frames[source]
    margin = (WINDOW - 1) * SPAN
    keys_padded = jnp.concatenate([jnp.zeros((margin, KW), keys.dtype), keys], axis=0)
    values_padded = jnp.concatenate([jnp.zeros((margin, KW), values.dtype), values], axis=0)
    clips_padded = jnp.concatenate([jnp.full((margin,), -1, jnp.int32), segments.astype(jnp.int32)], axis=0)
    groups = Q_HEADS // KV_HEADS
    inverse_root = 1.0 / math.sqrt(HEAD_DIM)

    def one_block(block_number):
        first = (block_number * SPAN).astype(jnp.int32)
        query_block = lax.dynamic_slice_in_dim(queries, first, SPAN, 0).astype(jnp.float32).reshape(SPAN, KV_HEADS, groups, HEAD_DIM)
        key_block = lax.dynamic_slice_in_dim(keys_padded, first, WINDOW * SPAN, 0).astype(jnp.float32).reshape(WINDOW * SPAN, KV_HEADS, HEAD_DIM)
        value_block = lax.dynamic_slice_in_dim(values_padded, first, WINDOW * SPAN, 0).astype(jnp.float32).reshape(WINDOW * SPAN, KV_HEADS, HEAD_DIM)
        query_clip = lax.dynamic_slice_in_dim(segments.astype(jnp.int32), first, SPAN, 0)
        key_clip = lax.dynamic_slice_in_dim(clips_padded, first, WINDOW * SPAN, 0)
        query_place = first + jnp.arange(SPAN, dtype=jnp.int32)
        key_place = first - margin + jnp.arange(WINDOW * SPAN, dtype=jnp.int32)
        allowed = (key_place[None, :] <= query_place[:, None]) & (key_clip[None, :] == query_clip[:, None])
        scores = jnp.einsum('qhgd,khd->hgqk', query_block, key_block) * inverse_root
        masked = jnp.where(allowed, scores, -jnp.inf)
        highest = lax.optimization_barrier(jnp.max(masked, axis=-1, keepdims=True))
        weights = jnp.where(allowed, jnp.exp(masked - highest), 0.0)
        totals = lax.optimization_barrier(jnp.sum(weights, axis=-1))
        rounded = lax.optimization_barrier(weights.astype(jnp.bfloat16)).astype(jnp.float32)
        summed = jnp.einsum('hgqk,khd->qhgd', rounded, value_block)
        result = summed / jnp.transpose(totals, (2, 0, 1))[..., None]
        return result.reshape(SPAN, QW).astype(jnp.bfloat16)
    blocks = lax.map(one_block, jnp.arange(CYCLE, dtype=jnp.int32))
    return blocks.reshape(SEQ_LEN, QW)
```

```python
import functools
import math

import jax
import jax.numpy as jnp
from jax import lax
from jax.experimental import pallas as pl
from jax.experimental.pallas import tpu as pltpu
from jax.sharding import PartitionSpec as P

KV_HEADS = 4
HEAD_DIM = 128
SPAN = 256
WINDOW = 5
X, Z = 4, 16
MESH = pl.DeviceIdType.MESH
SCALE = math.log2(math.e) / math.sqrt(HEAD_DIM)
MASKED = -1e30
BF16, F32, I32 = jnp.bfloat16, jnp.float32, jnp.int32


def kernel(
    q_hbm,
    k_hbm,
    v_hbm,
    count_ref,
    seg_hbm,
    out_hbm,
    qf,
    kvf,
    seg,
    count,
    count_prev,
    count_pair,
    pair_sum,
    column,
    column_sum,
    columns,
    base,
    base_in,
    before,
    before_in,
    lead,
    turn,
    kv_tail,
    kv_tail_in,
    q_tail,
    q_tail_in,
    kv,
    qr,
    bias,
    out,
    acc,
    top,
    total,
    load_sem,
    seg_sem,
    out_sem,
    one_send,
    one_recv,
    z_send,
    z_recv,
    x_send,
    x_recv,
    tail_send,
    tail_recv,
    block_send,
    block_recv,
):
    n = lax.axis_size("seq")
    d = lax.axis_index("seq")
    core = lax.rem(d, 2)
    chip = d // 2
    z = lax.rem(chip, Z)
    x = chip // Z
    heads = qr.shape[0] // KV_HEADS
    wide = heads * HEAD_DIM

    def at(index):
        return {"seq": lax.rem(index + n, n)}

    follower = at(d + 1)
    onward = at(d + 2)
    partner = at(d + 1 - 2 * core)

    def remote(src, dst, send, recv, device):
        return pltpu.make_async_remote_copy(
            src_ref=src,
            dst_ref=dst,
            send_sem=send,
            recv_sem=recv,
            device_id=device,
            device_id_type=MESH,
        )

    def z_peer(k):
        return at(x * (2 * Z) + 2 * lax.rem(z + k, Z) + core)

    def x_peer(k):
        return at(lax.rem(x + k, X) * (2 * Z) + 2 * z + core)

    loads = []
    for g in range(KV_HEADS):
        columns_of = pl.ds(g * HEAD_DIM, HEAD_DIM)
        for part, src in enumerate((k_hbm, v_hbm)):
            loads.append(
                pltpu.make_async_copy(
                    src.at[:, columns_of],
                    kvf.at[g, :, pl.ds(part * HEAD_DIM, HEAD_DIM)],
                    load_sem.at[2 * g + part],
                )
            )
    q_loads = [
        pltpu.make_async_copy(
            q_hbm.at[:, pl.ds(g * wide, wide)],
            qf.at[g],
            load_sem.at[2 * KV_HEADS + g],
        )
        for g in range(KV_HEADS)
    ]
    seg_load = pltpu.make_async_copy(seg_hbm, seg, seg_sem)
    for load in loads + q_loads + [seg_load]:
        load.start()

    barrier = pltpu.get_barrier_semaphore()

    def greet(device):
        pl.semaphore_signal(barrier, inc=1, device_id=device, device_id_type=MESH)

    greet(partner)
    greet(at(d + 2))
    greet(at(d - 2))

    @pl.when(core == 1)
    def _():
        greet(at(d + 1))

    @pl.when(core == 0)
    def _():
        greet(at(d - 1))
        lax.fori_loop(1, Z, lambda k, _: greet(z_peer(k)), None)
        lax.fori_loop(1, X, lambda k, _: greet(x_peer(k)), None)

    own_count = count_ref[0]
    count[...] = jnp.full(count.shape, own_count.astype(F32))
    for load in loads:
        load.wait()

    high = own_count - SPAN
    for g in range(KV_HEADS):
        slot = lax.broadcasted_iota(I32, (SPAN, 2 * HEAD_DIM), 0)
        kv_tail[g] = jnp.where(slot < high, kvf[g, SPAN:, :], kvf[g, :SPAN, :])

    def select_q(g):
        q_loads[g].wait()
        slot = lax.broadcasted_iota(I32, (SPAN, wide), 0)
        q_tail[g] = jnp.where(slot < high, qf[g, SPAN:, :], qf[g, :SPAN, :])

    select_q(0)
    pl.semaphore_wait(barrier, jnp.where(core == 0, Z + X + 2, 4))

    count_copy = remote(count, count_prev, one_send.at[0], one_recv.at[0], follower)
    pair_copy = remote(count, count_pair, one_send.at[1], one_recv.at[1], partner)
    before_copy = remote(before, before_in, one_send.at[2], one_recv.at[2], partner)
    has_next, has_prev = d < n - 1, d > 0
    has_onward, has_back = d < n - 2, d > 1

    def start_if(there, copy):
        pl.when(there)(copy.start)

    start_if(has_next, count_copy)
    start_if(core == 1, pair_copy)

    kv_tails = [
        remote(kv_tail.at[g], kv_tail_in.at[g], tail_send.at[g], tail_recv.at[g], follower)
        for g in range(KV_HEADS)
    ]
    q_tails = [
        remote(
            q_tail.at[g],
            q_tail_in.at[g],
            tail_send.at[KV_HEADS + g],
            tail_recv.at[KV_HEADS + g],
            follower,
        )
        for g in range(KV_HEADS)
    ]
    for g in range(KV_HEADS):
        start_if(has_next, kv_tails[g])
    select_q(1)
    start_if(has_next, q_tails[0])
    select_q(2)
    start_if(has_next, q_tails[1])
    select_q(3)
    pl.when(has_prev)(count_copy.wait_recv)

    @pl.when(d == 0)
    def _():
        count_prev[...] = jnp.full(count_prev.shape, float(SPAN), F32)
        kv_tail_in[...] = jnp.zeros(kv_tail_in.shape, BF16)
        q_tail_in[...] = jnp.zeros(q_tail_in.shape, BF16)

    @pl.when(d < 2)
    def _():
        for t in (2, 4):
            kv[:, t] = jnp.zeros((KV_HEADS, *kv.shape[2:]), BF16)

    @pl.when(core == 0)
    def _():
        pair_copy.wait_recv()
        pair_sum[...] = count[...] + count_pair[...]
        column[pl.ds(z, 1)] = pair_sum[...][None]

        def z_copy(k):
            return remote(pair_sum, column.at[z], z_send.at[k], z_recv.at[z], z_peer(k))

        def z_from(k):
            other = lax.rem(z + k, Z)
            return remote(
                pair_sum, column.at[other], z_send.at[k], z_recv.at[other], z_peer(k)
            )

        lax.fori_loop(1, Z, lambda k, _: z_copy(k).start(), None)
        lax.fori_loop(1, Z, lambda k, _: z_from(k).wait_recv(), None)
        z_place = lax.broadcasted_iota(I32, column.shape, 0)
        x_place = lax.broadcasted_iota(I32, columns.shape, 0)
        base_copy = remote(base, base_in, one_send.at[3], one_recv.at[3], z_peer(Z - 1))

        def x_copy(k):
            return remote(column_sum, columns.at[x], x_send.at[k], x_recv.at[x], x_peer(k))

        def x_from(k):
            other = lax.rem(x + k, X)
            return remote(
                column_sum, columns.at[other], x_send.at[k], x_recv.at[other], x_peer(k)
            )

        @pl.when(z > 0)
        def _():
            column_sum[...] = jnp.sum(column[...], axis=0)
            columns[pl.ds(x, 1)] = column_sum[...][None]
            for k in range(1, X):
                x_copy(k).start()
            for k in range(1, X):
                x_from(k).wait_recv()
            base[...] = jnp.sum(jnp.where(x_place < x, columns[...], 0.0), axis=0)
            pl.when(z == 1)(base_copy.start)
            before[...] = base[...] + jnp.sum(jnp.where(z_place < z, column[...], 0.0), axis=0)

        @pl.when(z == 0)
        def _():
            base_copy.wait_recv()
            before[...] = base_in[...]

        before_copy.start()
        lead[...] = before[...] - (d * SPAN).astype(F32)
        lax.fori_loop(1, Z, lambda k, _: z_copy(k).wait_send(), None)

        @pl.when(z > 0)
        def _():
            for k in range(1, X):
                x_copy(k).wait_send()

        pl.when(z == 1)(base_copy.wait_send)
        before_copy.wait_send()

    @pl.when(core == 1)
    def _():
        before_copy.wait_recv()
        lead[...] = before_in[...] + count_prev[...] - (d * SPAN).astype(F32)
        pair_copy.wait_send()

    lead_in = lead[0:1, :].astype(I32)
    lead_before = (lead[0:1, :] - count_prev[0:1, :]).astype(I32)
    place = lax.broadcasted_iota(I32, (SPAN, SPAN), 0)
    slot = lax.broadcasted_iota(I32, (SPAN, SPAN), 1)
    step = place - slot
    arrived = (((step - lead_before) & (SPAN - 1)) == 0) & (place < lead_in)
    turn[:, :SPAN] = jnp.where(arrived, 1.0, 0.0).astype(BF16)
    turn[:, SPAN:] = jnp.where(step == lead_in, 1.0, 0.0).astype(BF16)

    def turned(tail, own):
        rows = jnp.dot(turn[:, :SPAN], tail, preferred_element_type=F32)
        rows += jnp.dot(turn[:, SPAN:], own, preferred_element_type=F32)
        return rows.astype(BF16)

    def hop(g, source, target, device):
        return remote(
            kv.at[g, source],
            kv.at[g, target],
            block_send.at[g, target],
            block_recv.at[g, target],
            device,
        )

    def arrival(g, target):
        hop(g, target, target, partner).wait_recv()

    for g in range(KV_HEADS):
        pl.when(has_prev)(kv_tails[g].wait_recv)
        kv[g, 0] = turned(kv_tail_in[g], kvf[g, :SPAN, :])

    seg_load.wait()
    both = HEAD_DIM

    def clip_row(block):
        row = 2 * jnp.maximum(block, 0)
        return jnp.concatenate([seg[pl.ds(row, 1), :], seg[pl.ds(row + 1, 1), :]], axis=1).astype(F32)

    query_clip = jnp.broadcast_to(clip_row(d), (SPAN, SPAN)).T
    for t in range(WINDOW):
        same = query_clip == clip_row(d - t)
        if t == 0:
            same = same & (slot <= place)
        there = jnp.where(d >= t, 0.0, MASKED)
        bias[:, pl.ds(t * SPAN, SPAN)] = jnp.where(same, 0.0, MASKED) + there

    def send_own(g):
        start_if(has_onward, hop(g, 0, 2, onward))

        @pl.when(core == 0)
        def _():
            hop(g, 0, 1, partner).start()

    def forward(g):
        pl.when(has_back)(lambda: arrival(g, 2))
        start_if(has_onward, hop(g, 2, 4, onward))

        @pl.when(core == 0)
        def _():
            hop(g, 2, 3, partner).start()

        @pl.when(core == 1)
        def _():
            hop(g, 2, 1, partner).start()

    def forward_far(g):
        pl.when(has_back)(lambda: arrival(g, 4))

        @pl.when(core == 1)
        def _():
            hop(g, 4, 3, partner).start()

    send_own(0)
    send_own(1)
    start_if(has_next, q_tails[2])
    send_own(2)
    send_own(3)
    start_if(has_next, q_tails[3])

    def turn_q(g):
        pl.when(has_prev)(q_tails[g].wait_recv)
        rows = turned(q_tail_in[g], qf[g, :SPAN, :])
        for h in range(heads):
            qr[g * heads + h] = rows[:, h * HEAD_DIM : (h + 1) * HEAD_DIM]

    def attend(g, first, end, opening, closing):
        span = (end - first) * SPAN

        def head(h, _):
            i = g * heads + h
            keys = kv[g, first:end, :, :HEAD_DIM].reshape(span, HEAD_DIM)
            values = kv[g, first:end, :, HEAD_DIM:].reshape(span, HEAD_DIM)
            scores = lax.dot_general(
                qr[i], keys, (((1,), (1,)), ((), ())), preferred_element_type=F32
            )
            scores = scores * SCALE + bias[:, first * SPAN : end * SPAN]
            peak = jnp.max(scores, axis=1, keepdims=True)
            if not opening:
                old = top[i]
                peak = jnp.maximum(peak, old[:, :1])
            weights = jnp.exp2(scores - peak)
            sums = jnp.sum(weights, axis=1, keepdims=True)
            product = jnp.dot(weights.astype(BF16), values, preferred_element_type=F32)
            if not opening:
                factor = jnp.exp2(old - peak)
                sums = sums + total[i] * factor
                product = product + acc[i] * factor
            if closing:
                out[g, :, pl.ds(pl.multiple_of(h * HEAD_DIM, HEAD_DIM), HEAD_DIM)] = (
                    product / sums
                ).astype(BF16)
            else:
                top[i] = jnp.broadcast_to(peak, (SPAN, HEAD_DIM))
                total[i] = jnp.broadcast_to(sums, (SPAN, HEAD_DIM))
                acc[i] = product
            return 0

        lax.fori_loop(0, heads, head, 0)

    def out_copy(g):
        return pltpu.make_async_copy(
            out.at[g], out_hbm.at[:, pl.ds(g * wide, wide)], out_sem.at[g]
        )

    for g in range(KV_HEADS):
        forward(g)
    for g in range(KV_HEADS):
        turn_q(g)
        forward_far(g)
        arrival(g, 1)
        arrival(g, 3)
        attend(g, 0, WINDOW, True, True)
        out_copy(g).start()

    for g in range(KV_HEADS):
        out_copy(g).wait()
        pl.when(has_next)(kv_tails[g].wait_send)
        pl.when(has_next)(q_tails[g].wait_send)
        pl.when(has_onward)(hop(g, 0, 2, onward).wait_send)
        pl.when(has_onward)(hop(g, 2, 4, onward).wait_send)
        hop(g, 2, 3, partner).wait_send()

        @pl.when(core == 0)
        def _():
            hop(g, 0, 1, partner).wait_send()

        @pl.when(core == 1)
        def _():
            hop(g, 2, 1, partner).wait_send()

    pl.when(has_next)(count_copy.wait_send)


def shards(query_frames, key_frames, value_frames, token_counts, segments):
    slots, qw = query_frames.shape
    heads = qw // HEAD_DIM
    wide = qw // KV_HEADS
    any_space = pl.BlockSpec(memory_space=pl.ANY)
    lanes = 2 * HEAD_DIM
    small = pltpu.VMEM((8, SPAN), F32)
    dma = pltpu.SemaphoreType.DMA
    return pl.pallas_call(
        kernel,
        out_shape=jax.ShapeDtypeStruct((SPAN, qw), BF16),
        in_specs=[any_space, any_space, any_space, pl.BlockSpec(memory_space=pltpu.SMEM), any_space],
        out_specs=any_space,
        scratch_shapes=[
            pltpu.VMEM((KV_HEADS, slots, wide), BF16),
            pltpu.VMEM((KV_HEADS, slots, lanes), BF16),
            pltpu.VMEM((segments.shape[0] // HEAD_DIM, HEAD_DIM), I32),
            small,
            small,
            small,
            small,
            pltpu.VMEM((Z, 8, SPAN), F32),
            small,
            pltpu.VMEM((X, 8, SPAN), F32),
            small,
            small,
            small,
            small,
            small,
            pltpu.VMEM((SPAN, 2 * SPAN), BF16),
            pltpu.VMEM((KV_HEADS, SPAN, lanes), BF16),
            pltpu.VMEM((KV_HEADS, SPAN, lanes), BF16),
            pltpu.VMEM((KV_HEADS, SPAN, wide), BF16),
            pltpu.VMEM((KV_HEADS, SPAN, wide), BF16),
            pltpu.VMEM((KV_HEADS, WINDOW, SPAN, lanes), BF16),
            pltpu.VMEM((heads, SPAN, HEAD_DIM), BF16),
            pltpu.VMEM((SPAN, WINDOW * SPAN), F32),
            pltpu.VMEM((KV_HEADS, SPAN, wide), BF16),
            pltpu.VMEM((heads, SPAN, HEAD_DIM), F32),
            pltpu.VMEM((heads, SPAN, HEAD_DIM), F32),
            pltpu.VMEM((heads, SPAN, HEAD_DIM), F32),
            dma((3 * KV_HEADS,)),
            dma,
            dma((KV_HEADS,)),
            dma((4,)),
            dma((4,)),
            dma((Z,)),
            dma((Z,)),
            dma((X,)),
            dma((X,)),
            dma((2 * KV_HEADS,)),
            dma((2 * KV_HEADS,)),
            dma((KV_HEADS, WINDOW)),
            dma((KV_HEADS, WINDOW)),
        ],
        compiler_params=pltpu.CompilerParams(
            collective_id=0, has_side_effects=True, vmem_limit_bytes=62 * 2**20
        ),
    )(query_frames, key_frames, value_frames, token_counts, segments.reshape(-1, HEAD_DIM))


def solution(mesh):
    share = P(("group", "seq"), None)
    return jax.shard_map(
        shards,
        mesh=mesh,
        in_specs=(share, share, share, P(("group", "seq")), P("group")),
        out_specs=share,
        check_vma=False,
    )
```

```python
import functools
import math

import jax
import jax.numpy as jnp
from jax import lax
from jax.experimental import pallas as pl
from jax.experimental.pallas import tpu as pltpu
from jax.sharding import PartitionSpec as P

KV_HEADS = 4
HEAD_DIM = 128
SPAN = 256
WINDOW = 5
X, Z = 4, 16
HELD = 2
RELAYED = 8
FIRST_RELAY, SECOND_RELAY = 2 * (Z - 1) // 3, (Z - 1) // 3
MESH = pl.DeviceIdType.MESH
SCALE = math.log2(math.e) / math.sqrt(HEAD_DIM)
MASKED = -1e30
BF16, F32, I32 = jnp.bfloat16, jnp.float32, jnp.int32


def kernel(
    q_hbm,
    k_hbm,
    v_hbm,
    count_ref,
    seg_hbm,
    out_hbm,
    qf,
    kvf,
    seg,
    count,
    count_prev,
    count_pair,
    pair_sum,
    column,
    column_sum,
    columns,
    base,
    base_in,
    before,
    before_in,
    lead,
    turn,
    kv_tail,
    kv_tail_in,
    q_tail,
    q_tail_in,
    kv,
    qr,
    bias,
    out,
    acc,
    top,
    total,
    relay,
    load_sem,
    seg_sem,
    out_sem,
    one_send,
    one_recv,
    z_send,
    z_recv,
    x_send,
    x_recv,
    tail_send,
    tail_recv,
    block_send,
    block_recv,
    relay_send,
    relay_recv,
):
    n = lax.axis_size("seq")
    d = lax.axis_index("seq")
    core = lax.rem(d, 2)
    chip = d // 2
    z = lax.rem(chip, Z)
    x = chip // Z
    heads = qr.shape[0] // KV_HEADS
    wide = heads * HEAD_DIM

    def at(index):
        return {"seq": lax.rem(index + n, n)}

    follower = at(d + 1)
    onward = at(d + 2)
    partner = at(d + 1 - 2 * core)

    def remote(src, dst, send, recv, device):
        return pltpu.make_async_remote_copy(
            src_ref=src,
            dst_ref=dst,
            send_sem=send,
            recv_sem=recv,
            device_id=device,
            device_id_type=MESH,
        )

    def z_peer(k):
        return at(x * (2 * Z) + 2 * lax.rem(z + k, Z) + core)

    def x_peer(k):
        return at(lax.rem(x + k, X) * (2 * Z) + 2 * z + core)

    loads = []
    for g in range(KV_HEADS):
        columns_of = pl.ds(g * HEAD_DIM, HEAD_DIM)
        for part, src in enumerate((k_hbm, v_hbm)):
            loads.append(
                pltpu.make_async_copy(
                    src.at[:, columns_of],
                    kvf.at[g, :, pl.ds(part * HEAD_DIM, HEAD_DIM)],
                    load_sem.at[2 * g + part],
                )
            )
    q_loads = [
        pltpu.make_async_copy(
            q_hbm.at[:, pl.ds(g * wide, wide)],
            qf.at[g],
            load_sem.at[2 * KV_HEADS + g],
        )
        for g in range(KV_HEADS)
    ]
    seg_load = pltpu.make_async_copy(seg_hbm, seg, seg_sem)
    for load in loads + q_loads + [seg_load]:
        load.start()

    barrier = pltpu.get_barrier_semaphore()

    def greet(device):
        pl.semaphore_signal(barrier, inc=1, device_id=device, device_id_type=MESH)

    has_next, has_prev = d < n - 1, d > 0
    has_onward, has_back = d < n - 2, d > 1
    turning = x < X - 1
    source = (core == 1) & turning & (z == Z - 1)
    first_relay = (core == 1) & turning & (z == FIRST_RELAY)
    second_relay = (core == 1) & (x > 0) & (z == SECOND_RELAY)
    sink = (core == 0) & (x > 0) & (z == 0)

    def in_column(column_x, column_z, column_core):
        return at((column_x * Z + column_z) * 2 + column_core)

    pl.when(d > 0)(lambda: greet(partner))
    pl.when(has_back)(lambda: greet(at(d - 2)))
    sends_on = jnp.where(has_onward, 1, 0)
    first_chip = chip == 0

    @pl.when(core == 0)
    def _():
        pl.when(has_prev)(lambda: greet(at(d - 1)))
        lax.fori_loop(1, Z, lambda k, _: greet(z_peer(k)), None)
        lax.fori_loop(1, X, lambda k, _: greet(x_peer(k)), None)

    pl.when(first_relay)(lambda: greet(in_column(x, Z - 1, 1)))
    pl.when(second_relay)(lambda: greet(in_column(x - 1, FIRST_RELAY, 1)))
    pl.when(sink)(lambda: greet(in_column(x, SECOND_RELAY, 1)))

    own_count = count_ref[0]
    count[...] = jnp.full(count.shape, own_count.astype(F32))

    count_copy = remote(count, count_prev, one_send.at[0], one_recv.at[0], follower)
    pair_copy = remote(count, count_pair, one_send.at[1], one_recv.at[1], partner)
    before_copy = remote(before, before_in, one_send.at[2], one_recv.at[2], partner)

    def zero(ref):
        ref[...] = jnp.zeros(ref.shape, ref.dtype)

    def start_if(there, copy):
        pl.when(there)(copy.start)

    @pl.when(core == 1)
    def _():
        also = jnp.where(source | first_relay | second_relay, 1, 0)
        beside = jnp.where(first_chip, 0, 1)
        pl.semaphore_wait(barrier, beside + jnp.where(has_next, 1, 0) + sends_on + also)
        start_if(jnp.logical_not(first_chip), pair_copy)
        start_if(has_next, count_copy)

    for load in loads:
        load.wait()

    high = own_count - SPAN
    for g in range(KV_HEADS):
        slot = lax.broadcasted_iota(I32, (SPAN, 2 * HEAD_DIM), 0)
        kv_tail[g] = jnp.where(slot < high, kvf[g, SPAN:, :], kvf[g, :SPAN, :])

    def select_q(g):
        q_loads[g].wait()
        slot = lax.broadcasted_iota(I32, (SPAN, wide), 0)
        q_tail[g] = jnp.where(slot < high, qf[g, SPAN:, :], qf[g, :SPAN, :])

    def kv_tail_copy(g):
        return remote(kv_tail.at[g], kv_tail_in.at[g], tail_send.at[g], tail_recv.at[g], follower)

    def q_tail_copy(g):
        return remote(
            q_tail.at[g],
            q_tail_in.at[g],
            tail_send.at[KV_HEADS + g],
            tail_recv.at[KV_HEADS + g],
            follower,
        )

    early = (core == 1) & (z < Z // 2)
    late = (core == 1) & (z >= Z // 2) & has_next & jnp.logical_not(source)
    piece = relay.shape[1]
    pieces = SPAN // piece

    def tail_piece(ref, j):
        return ref.at[HELD + j // pieces, pl.ds(lax.rem(j, pieces) * piece, piece)]

    def relay_in(j, device):
        return remote(tail_piece(q_tail, j), relay.at[j], relay_send.at[j], relay_recv.at[j], device)

    def relay_on(j, device):
        return remote(relay.at[j], relay.at[j], relay_send.at[j], relay_recv.at[j], device)

    def relay_out(j, device):
        arrived = tail_recv.at[KV_HEADS + HELD + j // pieces]
        return remote(relay.at[j], tail_piece(q_tail_in, j), relay_send.at[j], arrived, device)

    select_q(0)

    @pl.when(core == 1)
    def _():
        for g in range(KV_HEADS):
            start_if(has_next, kv_tail_copy(g))

    select_q(1)
    start_if((core == 1) & has_next, q_tail_copy(0))
    select_q(2)
    start_if((core == 1) & has_next, q_tail_copy(1))
    select_q(3)

    @pl.when(early)
    def _():
        for g in range(HELD, KV_HEADS):
            q_tail_copy(g).start()

    @pl.when(source)
    def _():
        to = in_column(x, FIRST_RELAY, 1)
        lax.fori_loop(0, RELAYED, lambda j, _: relay_in(j, to).start(), None)

    @pl.when(first_relay)
    def _():
        to = in_column(x + 1, SECOND_RELAY, 1)

        def pass_on(j, _):
            relay_on(j, to).wait_recv()
            relay_on(j, to).start()

        lax.fori_loop(0, RELAYED, pass_on, None)

    @pl.when(second_relay)
    def _():
        to = in_column(x, 0, 0)

        def pass_out(j, _):
            relay_on(j, to).wait_recv()
            relay_out(j, to).start()

        lax.fori_loop(0, RELAYED, pass_out, None)

    @pl.when(core == 0)
    def _():
        pl.semaphore_wait(barrier, Z + X - 1 + sends_on)
        count_copy.start()

    @pl.when(d == 0)
    def _():
        count_prev[...] = jnp.full(count_prev.shape, float(SPAN), F32)
        kv_tail_in[...] = jnp.zeros(kv_tail_in.shape, BF16)
        q_tail_in[...] = jnp.zeros(q_tail_in.shape, BF16)

    @pl.when(d < 2)
    def _():
        for t in (2, 4):
            kv[:, t] = jnp.zeros((KV_HEADS, *kv.shape[2:]), BF16)

    @pl.when(core == 0)
    def _():
        @pl.when(first_chip)
        def _():
            count_pair[...] = jnp.zeros(count_pair.shape, F32)

        pl.when(jnp.logical_not(first_chip))(pair_copy.wait_recv)
        pair_sum[...] = count[...] + count_pair[...]
        column[pl.ds(z, 1)] = pair_sum[...][None]

        def z_copy(k):
            return remote(pair_sum, column.at[z], z_send.at[k], z_recv.at[z], z_peer(k))

        def z_from(k):
            other = lax.rem(z + k, Z)
            return remote(
                pair_sum, column.at[other], z_send.at[k], z_recv.at[other], z_peer(k)
            )

        pl.when((x == 0) & (z > 0))(lambda: zero(column.at[0]))

        @pl.when(jnp.logical_not(first_chip))
        def _():
            lax.fori_loop(1, Z, lambda k, _: z_copy(k).start(), None)

        for g in range(KV_HEADS):
            kv_tail_copy(g).start()
            q_tail_copy(g).start()

        def z_arrival(k, _):
            pl.when((x > 0) | (lax.rem(z + k, Z) > 0))(z_from(k).wait_recv)

        lax.fori_loop(1, Z, z_arrival, None)
        z_place = lax.broadcasted_iota(I32, column.shape, 0)
        x_place = lax.broadcasted_iota(I32, columns.shape, 0)
        base_copy = remote(base, base_in, one_send.at[3], one_recv.at[3], z_peer(Z - 1))

        def x_copy(k):
            return remote(column_sum, columns.at[x], x_send.at[k], x_recv.at[x], x_peer(k))

        def x_from(k):
            other = lax.rem(x + k, X)
            return remote(
                column_sum, columns.at[other], x_send.at[k], x_recv.at[other], x_peer(k)
            )

        pl.when(has_prev)(count_copy.wait_recv)

        @pl.when(z > 0)
        def _():
            column_sum[...] = jnp.sum(column[...], axis=0)
            columns[pl.ds(x, 1)] = column_sum[...][None]
            for k in range(1, X):
                x_copy(k).start()
            for k in range(1, X):
                x_from(k).wait_recv()
            base[...] = jnp.sum(jnp.where(x_place > x, columns[...], 0.0), axis=0)
            pl.when(z == 1)(base_copy.start)
            later = jnp.sum(jnp.where(z_place >= z, column[...], 0.0), axis=0)
            before[...] = float(n * SPAN) - (base[...] + later)

        @pl.when(z == 0)
        def _():
            base_copy.wait_recv()
            later = base_in[...] + jnp.sum(column[...], axis=0)
            before[...] = jnp.where(first_chip, 0.0, float(n * SPAN) - later)

        before_copy.start()
        lead[...] = before[...] - (d * SPAN).astype(F32)

        @pl.when(jnp.logical_not(first_chip))
        def _():
            lax.fori_loop(1, Z, lambda k, _: z_copy(k).wait_send(), None)


        @pl.when(z > 0)
        def _():
            for k in range(1, X):
                x_copy(k).wait_send()

        pl.when(z == 1)(base_copy.wait_send)
        before_copy.wait_send()

    @pl.when(core == 1)
    def _():
        count_copy.wait_recv()
        before_copy.wait_recv()
        lead[...] = before_in[...] + count_prev[...] - (d * SPAN).astype(F32)
        pl.when(jnp.logical_not(first_chip))(pair_copy.wait_send)

    lead_in = lead[0:1, :].astype(I32)
    lead_before = (lead[0:1, :] - count_prev[0:1, :]).astype(I32)
    place = lax.broadcasted_iota(I32, (SPAN, SPAN), 0)
    slot = lax.broadcasted_iota(I32, (SPAN, SPAN), 1)
    step = place - slot
    arrived = (((step - lead_before) & (SPAN - 1)) == 0) & (place < lead_in)
    turn[:, :SPAN] = jnp.where(arrived, 1.0, 0.0).astype(BF16)
    turn[:, SPAN:] = jnp.where(step == lead_in, 1.0, 0.0).astype(BF16)

    def turned(tail, own):
        rows = jnp.dot(turn[:, :SPAN], tail, preferred_element_type=F32)
        rows += jnp.dot(turn[:, SPAN:], own, preferred_element_type=F32)
        return rows.astype(BF16)

    def hop(g, source, target, device):
        return remote(
            kv.at[g, source],
            kv.at[g, target],
            block_send.at[g, target],
            block_recv.at[g, target],
            device,
        )

    def arrival(g, target):
        hop(g, target, target, partner).wait_recv()

    for g in range(KV_HEADS):
        pl.when(has_prev)(kv_tail_copy(g).wait_recv)
        kv[g, 0] = turned(kv_tail_in[g], kvf[g, :SPAN, :])

    seg_load.wait()
    both = HEAD_DIM

    def clip_row(block):
        row = 2 * jnp.maximum(block, 0)
        return jnp.concatenate([seg[pl.ds(row, 1), :], seg[pl.ds(row + 1, 1), :]], axis=1).astype(F32)

    query_clip = jnp.broadcast_to(clip_row(d), (SPAN, SPAN)).T
    for t in range(WINDOW):
        same = query_clip == clip_row(d - t)
        if t == 0:
            same = same & (slot <= place)
        there = jnp.where(d >= t, 0.0, MASKED)
        bias[:, pl.ds(t * SPAN, SPAN)] = jnp.where(same, 0.0, MASKED) + there

    def send_own(g):
        start_if(has_onward, hop(g, 0, 2, onward))

        @pl.when(core == 0)
        def _():
            hop(g, 0, 1, partner).start()

    def forward(g):
        pl.when(has_back)(lambda: arrival(g, 2))
        start_if(has_onward, hop(g, 2, 4, onward))

        @pl.when(core == 0)
        def _():
            hop(g, 2, 3, partner).start()

        @pl.when(core == 1)
        def _():
            hop(g, 2, 1, partner).start()

    def forward_far(g):
        pl.when(has_back)(lambda: arrival(g, 4))

        @pl.when(core == 1)
        def _():
            hop(g, 4, 3, partner).start()

    for g in range(KV_HEADS):
        send_own(g)

    @pl.when(late)
    def _():
        for g in range(HELD, KV_HEADS):
            q_tail_copy(g).start()

    def turn_q(g):
        pl.when(has_prev)(q_tail_copy(g).wait_recv)
        rows = turned(q_tail_in[g], qf[g, :SPAN, :])
        for h in range(heads):
            qr[g * heads + h] = rows[:, h * HEAD_DIM : (h + 1) * HEAD_DIM]

    def attend(g, first, end, opening, closing):
        span = (end - first) * SPAN

        def head(h, _):
            i = g * heads + h
            keys = kv[g, first:end, :, :HEAD_DIM].reshape(span, HEAD_DIM)
            values = kv[g, first:end, :, HEAD_DIM:].reshape(span, HEAD_DIM)
            scores = lax.dot_general(
                qr[i], keys, (((1,), (1,)), ((), ())), preferred_element_type=F32
            )
            scores = scores * SCALE + bias[:, first * SPAN : end * SPAN]
            peak = jnp.max(scores, axis=1, keepdims=True)
            if not opening:
                old = top[i]
                peak = jnp.maximum(peak, old[:, :1])
            weights = jnp.exp2(scores - peak)
            sums = jnp.sum(weights, axis=1, keepdims=True)
            product = jnp.dot(weights.astype(BF16), values, preferred_element_type=F32)
            if not opening:
                factor = jnp.exp2(old - peak)
                sums = sums + total[i] * factor
                product = product + acc[i] * factor
            if closing:
                out[g, :, pl.ds(pl.multiple_of(h * HEAD_DIM, HEAD_DIM), HEAD_DIM)] = (
                    product / sums
                ).astype(BF16)
            else:
                top[i] = jnp.broadcast_to(peak, (SPAN, HEAD_DIM))
                total[i] = jnp.broadcast_to(sums, (SPAN, HEAD_DIM))
                acc[i] = product
            return 0

        lax.fori_loop(0, heads, head, 0, unroll=4)

    def out_copy(g):
        return pltpu.make_async_copy(
            out.at[g], out_hbm.at[:, pl.ds(g * wide, wide)], out_sem.at[g]
        )

    def own_step(g, _):
        turn_q(g)
        attend(g, 0, 1, True, False)

    def near_step(g, _):
        arrival(g, 1)
        attend(g, 1, 3, False, False)
        forward(g + HELD)

    def held_step(g, _):
        turn_q(g)
        arrival(g, 1)
        attend(g, 0, 3, True, False)

    def far_step(g, _):
        forward_far(g)
        arrival(g, 3)
        attend(g, 3, WINDOW, False, True)
        out_copy(g).start()

    lax.fori_loop(0, HELD, own_step, None)
    for g in range(HELD):
        forward(g)
    lax.fori_loop(0, HELD, near_step, None)
    lax.fori_loop(HELD, KV_HEADS, held_step, None)
    lax.fori_loop(0, KV_HEADS, far_step, None)

    for g in range(KV_HEADS):
        out_copy(g).wait()
        pl.when(has_next)(kv_tail_copy(g).wait_send)
        straight = has_next if g < HELD else has_next & jnp.logical_not(source)
        pl.when(straight)(q_tail_copy(g).wait_send)
        pl.when(has_onward)(hop(g, 0, 2, onward).wait_send)
        pl.when(has_onward)(hop(g, 2, 4, onward).wait_send)
        hop(g, 2, 3, partner).wait_send()

        @pl.when(core == 0)
        def _():
            hop(g, 0, 1, partner).wait_send()

        @pl.when(core == 1)
        def _():
            hop(g, 2, 1, partner).wait_send()

    pl.when(has_next)(count_copy.wait_send)

    @pl.when(source | first_relay | second_relay)
    def _():
        lax.fori_loop(0, RELAYED, lambda j, _: relay_on(j, partner).wait_send(), None)


def shards(query_frames, key_frames, value_frames, token_counts, segments):
    slots, qw = query_frames.shape
    heads = qw // HEAD_DIM
    wide = qw // KV_HEADS
    any_space = pl.BlockSpec(memory_space=pl.ANY)
    lanes = 2 * HEAD_DIM
    small = pltpu.VMEM((8, SPAN), F32)
    dma = pltpu.SemaphoreType.DMA
    return pl.pallas_call(
        kernel,
        out_shape=jax.ShapeDtypeStruct((SPAN, qw), BF16),
        in_specs=[any_space, any_space, any_space, pl.BlockSpec(memory_space=pltpu.SMEM), any_space],
        out_specs=any_space,
        scratch_shapes=[
            pltpu.VMEM((KV_HEADS, slots, wide), BF16),
            pltpu.VMEM((KV_HEADS, slots, lanes), BF16),
            pltpu.VMEM((segments.shape[0] // HEAD_DIM, HEAD_DIM), I32),
            small,
            small,
            small,
            small,
            pltpu.VMEM((Z, 8, SPAN), F32),
            small,
            pltpu.VMEM((X, 8, SPAN), F32),
            small,
            small,
            small,
            small,
            small,
            pltpu.VMEM((SPAN, 2 * SPAN), BF16),
            pltpu.VMEM((KV_HEADS, SPAN, lanes), BF16),
            pltpu.VMEM((KV_HEADS, SPAN, lanes), BF16),
            pltpu.VMEM((KV_HEADS, SPAN, wide), BF16),
            pltpu.VMEM((KV_HEADS, SPAN, wide), BF16),
            pltpu.VMEM((KV_HEADS, WINDOW, SPAN, lanes), BF16),
            pltpu.VMEM((heads, SPAN, HEAD_DIM), BF16),
            pltpu.VMEM((SPAN, WINDOW * SPAN), F32),
            pltpu.VMEM((KV_HEADS, SPAN, wide), BF16),
            pltpu.VMEM((heads, SPAN, HEAD_DIM), F32),
            pltpu.VMEM((heads, SPAN, HEAD_DIM), F32),
            pltpu.VMEM((heads, SPAN, HEAD_DIM), F32),
            pltpu.VMEM((RELAYED, (KV_HEADS - HELD) * SPAN // RELAYED, wide), BF16),
            dma((3 * KV_HEADS,)),
            dma,
            dma((KV_HEADS,)),
            dma((4,)),
            dma((4,)),
            dma((Z,)),
            dma((Z,)),
            dma((X,)),
            dma((X,)),
            dma((2 * KV_HEADS,)),
            dma((2 * KV_HEADS,)),
            dma((KV_HEADS, WINDOW)),
            dma((KV_HEADS, WINDOW)),
            dma((RELAYED,)),
            dma((RELAYED,)),
        ],
        compiler_params=pltpu.CompilerParams(
            collective_id=0, has_side_effects=True, vmem_limit_bytes=62 * 2**20
        ),
    )(query_frames, key_frames, value_frames, token_counts, segments.reshape(-1, HEAD_DIM))


def solution(mesh):
    share = P(("group", "seq"), None)
    return jax.shard_map(
        shards,
        mesh=mesh,
        in_specs=(share, share, share, P(("group", "seq")), P("group")),
        out_specs=share,
        check_vma=False,
    )
```

```python
import functools
import math

import jax
import jax.numpy as jnp
from jax import lax
from jax.experimental import pallas as pl
from jax.experimental.pallas import tpu as pltpu
from jax.sharding import PartitionSpec as P

KV_HEADS = 4
HEAD_DIM = 128
SPAN = 256
WINDOW = 5
X, Z = 4, 16
HELD = 2
RELAYED = 8
FIRST_RELAY, SECOND_RELAY = 2 * (Z - 1) // 3, (Z - 1) // 3
MESH = pl.DeviceIdType.MESH
SCALE = math.log2(math.e) / math.sqrt(HEAD_DIM)
MASKED = -1e30
BF16, F32, I32 = jnp.bfloat16, jnp.float32, jnp.int32


def kernel(
    q_hbm,
    k_hbm,
    v_hbm,
    count_ref,
    seg_hbm,
    out_hbm,
    qf,
    kvf,
    seg,
    count,
    count_prev,
    count_pair,
    pair_sum,
    column,
    column_sum,
    columns,
    base,
    base_in,
    before,
    before_in,
    lead,
    turn,
    kv_tail,
    kv_tail_in,
    q_tail,
    q_tail_in,
    kv,
    qr,
    bias,
    out,
    acc,
    top,
    total,
    relay,
    load_sem,
    seg_sem,
    out_sem,
    one_send,
    one_recv,
    z_send,
    z_recv,
    x_send,
    x_recv,
    tail_send,
    tail_recv,
    block_send,
    block_recv,
    relay_send,
    relay_recv,
):
    n = lax.axis_size("seq")
    d = lax.axis_index("seq")
    core = lax.rem(d, 2)
    chip = d // 2
    z = lax.rem(chip, Z)
    x = chip // Z
    heads = qr.shape[0] // KV_HEADS
    wide = heads * HEAD_DIM

    def at(index):
        return {"seq": lax.rem(index + n, n)}

    follower = at(d + 1)
    onward = at(d + 2)
    partner = at(d + 1 - 2 * core)

    def remote(src, dst, send, recv, device):
        return pltpu.make_async_remote_copy(
            src_ref=src,
            dst_ref=dst,
            send_sem=send,
            recv_sem=recv,
            device_id=device,
            device_id_type=MESH,
        )

    loads = []
    for g in range(KV_HEADS):
        columns_of = pl.ds(g * HEAD_DIM, HEAD_DIM)
        for part, src in enumerate((k_hbm, v_hbm)):
            loads.append(
                pltpu.make_async_copy(
                    src.at[:, columns_of],
                    kvf.at[g, :, pl.ds(part * HEAD_DIM, HEAD_DIM)],
                    load_sem.at[2 * g + part],
                )
            )
    q_loads = [
        pltpu.make_async_copy(
            q_hbm.at[:, pl.ds(g * wide, wide)],
            qf.at[g],
            load_sem.at[2 * KV_HEADS + g],
        )
        for g in range(KV_HEADS)
    ]
    seg_load = pltpu.make_async_copy(seg_hbm, seg, seg_sem)
    for load in loads + q_loads + [seg_load]:
        load.start()

    barrier = pltpu.get_barrier_semaphore()

    def greet(device):
        pl.semaphore_signal(barrier, inc=1, device_id=device, device_id_type=MESH)

    column[...] = jnp.zeros(column.shape, F32)
    columns[...] = jnp.zeros(columns.shape, F32)

    has_next, has_prev = d < n - 1, d > 0
    has_onward, has_back = d < n - 2, d > 1
    turning = x < X - 1
    source = (core == 1) & turning & (z == Z - 1)
    first_relay = (core == 1) & turning & (z == FIRST_RELAY)
    second_relay = (core == 1) & (x > 0) & (z == SECOND_RELAY)
    sink = (core == 0) & (x > 0) & (z == 0)

    def in_column(column_x, column_z, column_core):
        return at((column_x * Z + column_z) * 2 + column_core)

    pl.when(d > 0)(lambda: greet(partner))
    pl.when(has_back)(lambda: greet(at(d - 2)))
    sends_on = jnp.where(has_onward, 1, 0)
    first_chip = chip == 0
    below = (z == 0) & (x > 0)

    @pl.when(core == 0)
    def _():
        pl.when(has_prev)(lambda: greet(at(d - 1)))

        @pl.when(z > 0)
        def _():
            lax.fori_loop(z + 1, Z, lambda k, _: greet(in_column(x, k, 0)), None)

        pl.when((z > 1) | below)(lambda: greet(in_column(x, 1, 0)))

        @pl.when(z == 1)
        def _():
            pl.when(x > 0)(lambda: greet(in_column(x, 0, 0)))
            lax.fori_loop(x + 1, X, lambda k, _: greet(in_column(k, 1, 0)), None)

    pl.when(first_relay)(lambda: greet(in_column(x, Z - 1, 1)))
    pl.when(second_relay)(lambda: greet(in_column(x - 1, FIRST_RELAY, 1)))
    pl.when(sink)(lambda: greet(in_column(x, SECOND_RELAY, 1)))

    own_count = count_ref[0]
    count[...] = jnp.full(count.shape, own_count.astype(F32))

    count_copy = remote(count, count_prev, one_send.at[0], one_recv.at[0], follower)
    pair_copy = remote(count, count_pair, one_send.at[1], one_recv.at[1], partner)
    before_copy = remote(before, before_in, one_send.at[2], one_recv.at[2], partner)

    def zero(ref):
        ref[...] = jnp.zeros(ref.shape, ref.dtype)

    def start_if(there, copy):
        pl.when(there)(copy.start)

    @pl.when(core == 1)
    def _():
        also = jnp.where(source | first_relay | second_relay, 1, 0)
        beside = jnp.where(first_chip, 0, 1)
        pl.semaphore_wait(barrier, beside + jnp.where(has_next, 1, 0) + sends_on + also)
        start_if(jnp.logical_not(first_chip), pair_copy)
        start_if(has_next, count_copy)

    for load in loads:
        load.wait()

    high = own_count - SPAN
    for g in range(KV_HEADS):
        slot = lax.broadcasted_iota(I32, (SPAN, 2 * HEAD_DIM), 0)
        kv_tail[g] = jnp.where(slot < high, kvf[g, SPAN:, :], kvf[g, :SPAN, :])

    def select_q(g):
        q_loads[g].wait()
        slot = lax.broadcasted_iota(I32, (SPAN, wide), 0)
        q_tail[g] = jnp.where(slot < high, qf[g, SPAN:, :], qf[g, :SPAN, :])

    def kv_tail_copy(g):
        return remote(kv_tail.at[g], kv_tail_in.at[g], tail_send.at[g], tail_recv.at[g], follower)

    def q_tail_copy(g):
        return remote(
            q_tail.at[g],
            q_tail_in.at[g],
            tail_send.at[KV_HEADS + g],
            tail_recv.at[KV_HEADS + g],
            follower,
        )

    early = (core == 1) & (z < Z // 2)
    late = (core == 1) & (z >= Z // 2) & has_next & jnp.logical_not(source)
    piece = relay.shape[1]
    pieces = SPAN // piece

    def tail_piece(ref, j):
        return ref.at[HELD + j // pieces, pl.ds(lax.rem(j, pieces) * piece, piece)]

    def relay_in(j, device):
        return remote(tail_piece(q_tail, j), relay.at[j], relay_send.at[j], relay_recv.at[j], device)

    def relay_on(j, device):
        return remote(relay.at[j], relay.at[j], relay_send.at[j], relay_recv.at[j], device)

    def relay_out(j, device):
        arrived = tail_recv.at[KV_HEADS + HELD + j // pieces]
        return remote(relay.at[j], tail_piece(q_tail_in, j), relay_send.at[j], arrived, device)

    select_q(0)

    @pl.when(core == 1)
    def _():
        for g in range(KV_HEADS):
            start_if(has_next, kv_tail_copy(g))

    select_q(1)
    start_if((core == 1) & has_next, q_tail_copy(0))
    select_q(2)
    start_if((core == 1) & has_next, q_tail_copy(1))
    select_q(3)

    @pl.when(early)
    def _():
        for g in range(HELD, KV_HEADS):
            q_tail_copy(g).start()

    @pl.when(source)
    def _():
        to = in_column(x, FIRST_RELAY, 1)
        lax.fori_loop(0, RELAYED, lambda j, _: relay_in(j, to).start(), None)

    @pl.when(first_relay)
    def _():
        to = in_column(x + 1, SECOND_RELAY, 1)

        def pass_on(j, _):
            relay_on(j, to).wait_recv()
            relay_on(j, to).start()

        lax.fori_loop(0, RELAYED, pass_on, None)

    @pl.when(second_relay)
    def _():
        to = in_column(x, 0, 0)

        def pass_out(j, _):
            relay_on(j, to).wait_recv()
            relay_out(j, to).start()

        lax.fori_loop(0, RELAYED, pass_out, None)

    @pl.when(core == 0)
    def _():
        summing = jnp.where(z == 1, Z - 2 + jnp.minimum(x, 1) + x, jnp.maximum(z - 1, 0))
        pl.semaphore_wait(barrier, 1 + sends_on + summing + jnp.where(below, 1, 0))
        count_copy.start()

    @pl.when(d == 0)
    def _():
        count_prev[...] = jnp.full(count_prev.shape, float(SPAN), F32)
        kv_tail_in[...] = jnp.zeros(kv_tail_in.shape, BF16)
        q_tail_in[...] = jnp.zeros(q_tail_in.shape, BF16)

    @pl.when(d < 2)
    def _():
        for t in (2, 4):
            kv[:, t] = jnp.zeros((KV_HEADS, *kv.shape[2:]), BF16)

    @pl.when(core == 0)
    def _():
        @pl.when(first_chip)
        def _():
            count_pair[...] = jnp.zeros(count_pair.shape, F32)

        pl.when(jnp.logical_not(first_chip))(pair_copy.wait_recv)
        pair_sum[...] = count[...] + count_pair[...]
        column[pl.ds(z, 1)] = pair_sum[...][None]

        def pair_to(k):
            return remote(
                pair_sum, column.at[z], z_send.at[k], z_recv.at[z], in_column(x, k, 0)
            )

        def pair_from(k):
            return remote(
                pair_sum, column.at[k], z_send.at[k], z_recv.at[k], in_column(x, k, 0)
            )

        def column_to(k):
            return remote(
                column_sum, columns.at[x], x_send.at[k], x_recv.at[x], in_column(k, 1, 0)
            )

        def column_from(k):
            return remote(
                column_sum, columns.at[k], x_send.at[k], x_recv.at[k], in_column(k, 1, 0)
            )

        def base_to(k):
            return remote(base, base_in, z_send.at[k], one_recv.at[3], in_column(x, k, 0))

        base_below = remote(base_in, base_in, z_send.at[0], one_recv.at[3], in_column(x, 0, 0))

        lax.fori_loop(1, z, lambda k, _: pair_to(k).start(), None)
        pl.when(below)(lambda: pair_to(1).start())
        for g in range(KV_HEADS):
            kv_tail_copy(g).start()
            q_tail_copy(g).start()

        @pl.when(z > 0)
        def _():
            lax.fori_loop(z + 1, Z, lambda k, _: pair_from(k).wait_recv(), None)

        z_place = lax.broadcasted_iota(I32, column.shape, 0)
        x_place = lax.broadcasted_iota(I32, columns.shape, 0)
        rows = float(n * SPAN)

        @pl.when(z == 1)
        def _():
            pl.when(x > 0)(lambda: pair_from(0).wait_recv())
            column_sum[...] = jnp.sum(column[...], axis=0)
            lax.fori_loop(0, x, lambda k, _: column_to(k).start(), None)
            lax.fori_loop(x + 1, X, lambda k, _: column_from(k).wait_recv(), None)
            base[...] = jnp.sum(jnp.where(x_place > x, columns[...], 0.0), axis=0)
            base_in[...] = base[...] + column_sum[...]
            lax.fori_loop(2, Z, lambda k, _: base_to(k).start(), None)
            pl.when(x > 0)(base_below.start)
            later = jnp.sum(jnp.where(z_place >= z, column[...], 0.0), axis=0)
            before[...] = rows - (base[...] + later)

        @pl.when(z > 1)
        def _():
            base_to(z).wait_recv()
            later = jnp.sum(jnp.where(z_place >= z, column[...], 0.0), axis=0)
            before[...] = rows - (base_in[...] + later)

        @pl.when(below)
        def _():
            base_below.wait_recv()
            before[...] = rows - base_in[...]

        pl.when(first_chip)(lambda: zero(before))
        pl.when(has_prev)(count_copy.wait_recv)
        before_copy.start()
        lead[...] = before[...] - (d * SPAN).astype(F32)

        lax.fori_loop(1, z, lambda k, _: pair_to(k).wait_send(), None)
        pl.when(below)(lambda: pair_to(1).wait_send())

        @pl.when(z == 1)
        def _():
            lax.fori_loop(0, x, lambda k, _: column_to(k).wait_send(), None)
            lax.fori_loop(2, Z, lambda k, _: base_to(k).wait_send(), None)
            pl.when(x > 0)(base_below.wait_send)

        before_copy.wait_send()

    @pl.when(core == 1)
    def _():
        count_copy.wait_recv()
        before_copy.wait_recv()
        lead[...] = before_in[...] + count_prev[...] - (d * SPAN).astype(F32)
        pl.when(jnp.logical_not(first_chip))(pair_copy.wait_send)

    lead_in = lead[0:1, :].astype(I32)
    lead_before = (lead[0:1, :] - count_prev[0:1, :]).astype(I32)
    place = lax.broadcasted_iota(I32, (SPAN, SPAN), 0)
    slot = lax.broadcasted_iota(I32, (SPAN, SPAN), 1)
    step = place - slot
    arrived = (((step - lead_before) & (SPAN - 1)) == 0) & (place < lead_in)
    turn[:, :SPAN] = jnp.where(arrived, 1.0, 0.0).astype(BF16)
    turn[:, SPAN:] = jnp.where(step == lead_in, 1.0, 0.0).astype(BF16)

    def turned(tail, own):
        rows = jnp.dot(turn[:, :SPAN], tail, preferred_element_type=F32)
        rows += jnp.dot(turn[:, SPAN:], own, preferred_element_type=F32)
        return rows.astype(BF16)

    def hop(g, source, target, device):
        return remote(
            kv.at[g, source],
            kv.at[g, target],
            block_send.at[g, target],
            block_recv.at[g, target],
            device,
        )

    def arrival(g, target):
        hop(g, target, target, partner).wait_recv()

    for g in range(KV_HEADS):
        pl.when(has_prev)(kv_tail_copy(g).wait_recv)
        kv[g, 0] = turned(kv_tail_in[g], kvf[g, :SPAN, :])

    seg_load.wait()
    both = HEAD_DIM

    def clip_row(block):
        row = 2 * jnp.maximum(block, 0)
        return jnp.concatenate([seg[pl.ds(row, 1), :], seg[pl.ds(row + 1, 1), :]], axis=1).astype(F32)

    query_clip = jnp.broadcast_to(clip_row(d), (SPAN, SPAN)).T
    for t in range(WINDOW):
        same = query_clip == clip_row(d - t)
        if t == 0:
            same = same & (slot <= place)
        there = jnp.where(d >= t, 0.0, MASKED)
        bias[:, pl.ds(t * SPAN, SPAN)] = jnp.where(same, 0.0, MASKED) + there

    def send_own(g):
        start_if(has_onward, hop(g, 0, 2, onward))

        @pl.when(core == 0)
        def _():
            hop(g, 0, 1, partner).start()

    def forward(g):
        pl.when(has_back)(lambda: arrival(g, 2))
        start_if(has_onward, hop(g, 2, 4, onward))

        @pl.when(core == 0)
        def _():
            hop(g, 2, 3, partner).start()

        @pl.when(core == 1)
        def _():
            hop(g, 2, 1, partner).start()

    def forward_far(g):
        pl.when(has_back)(lambda: arrival(g, 4))

        @pl.when(core == 1)
        def _():
            hop(g, 4, 3, partner).start()

    for g in range(KV_HEADS):
        send_own(g)

    @pl.when(late)
    def _():
        for g in range(HELD, KV_HEADS):
            q_tail_copy(g).start()

    def turn_q(g):
        pl.when(has_prev)(q_tail_copy(g).wait_recv)
        rows = turned(q_tail_in[g], qf[g, :SPAN, :])
        for h in range(heads):
            qr[g * heads + h] = rows[:, h * HEAD_DIM : (h + 1) * HEAD_DIM]

    def attend(g, first, end, opening, closing):
        span = (end - first) * SPAN

        def head(h, _):
            i = g * heads + h
            keys = kv[g, first:end, :, :HEAD_DIM].reshape(span, HEAD_DIM)
            values = kv[g, first:end, :, HEAD_DIM:].reshape(span, HEAD_DIM)
            scores = lax.dot_general(
                qr[i], keys, (((1,), (1,)), ((), ())), preferred_element_type=F32
            )
            scores = scores * SCALE + bias[:, first * SPAN : end * SPAN]
            peak = jnp.max(scores, axis=1, keepdims=True)
            if not opening:
                old = top[i]
                peak = jnp.maximum(peak, old[:, :1])
            weights = jnp.exp2(scores - peak)
            sums = jnp.sum(weights, axis=1, keepdims=True)
            product = jnp.dot(weights.astype(BF16), values, preferred_element_type=F32)
            if not opening:
                factor = jnp.exp2(old - peak)
                sums = sums + total[i] * factor
                product = product + acc[i] * factor
            if closing:
                out[g, :, pl.ds(pl.multiple_of(h * HEAD_DIM, HEAD_DIM), HEAD_DIM)] = (
                    product / sums
                ).astype(BF16)
            else:
                top[i] = jnp.broadcast_to(peak, (SPAN, HEAD_DIM))
                total[i] = jnp.broadcast_to(sums, (SPAN, HEAD_DIM))
                acc[i] = product
            return 0

        lax.fori_loop(0, heads, head, 0, unroll=8)

    def out_copy(g):
        return pltpu.make_async_copy(
            out.at[g], out_hbm.at[:, pl.ds(g * wide, wide)], out_sem.at[g]
        )

    def own_step(g, _):
        turn_q(g)
        attend(g, 0, 1, True, False)

    def near_step(g, _):
        arrival(g, 1)
        attend(g, 1, 3, False, False)
        pl.when(z < Z - 1)(lambda: forward(g + HELD))

    def far_step(g, _):
        forward_far(g)
        arrival(g, 3)
        attend(g, 3, WINDOW, False, True)
        out_copy(g).start()

    def whole_step(g, _):
        turn_q(g)
        forward_far(g)
        arrival(g, 1)
        arrival(g, 3)
        attend(g, 0, WINDOW, True, True)
        out_copy(g).start()

    @pl.when(z == Z - 1)
    def _():
        for g in range(KV_HEADS):
            forward(g)

    lax.fori_loop(0, HELD, own_step, None)

    @pl.when(z < Z - 1)
    def _():
        for g in range(HELD):
            forward(g)

    lax.fori_loop(0, HELD, near_step, None)
    lax.fori_loop(0, HELD, far_step, None)
    lax.fori_loop(HELD, KV_HEADS, whole_step, None)

    for g in range(KV_HEADS):
        out_copy(g).wait()
        pl.when(has_next)(kv_tail_copy(g).wait_send)
        straight = has_next if g < HELD else has_next & jnp.logical_not(source)
        pl.when(straight)(q_tail_copy(g).wait_send)
        pl.when(has_onward)(hop(g, 0, 2, onward).wait_send)
        pl.when(has_onward)(hop(g, 2, 4, onward).wait_send)
        hop(g, 2, 3, partner).wait_send()

        @pl.when(core == 0)
        def _():
            hop(g, 0, 1, partner).wait_send()

        @pl.when(core == 1)
        def _():
            hop(g, 2, 1, partner).wait_send()

    pl.when(has_next)(count_copy.wait_send)

    @pl.when(source | first_relay | second_relay)
    def _():
        lax.fori_loop(0, RELAYED, lambda j, _: relay_on(j, partner).wait_send(), None)


def shards(query_frames, key_frames, value_frames, token_counts, segments):
    slots, qw = query_frames.shape
    heads = qw // HEAD_DIM
    wide = qw // KV_HEADS
    any_space = pl.BlockSpec(memory_space=pl.ANY)
    lanes = 2 * HEAD_DIM
    small = pltpu.VMEM((8, SPAN), F32)
    dma = pltpu.SemaphoreType.DMA
    return pl.pallas_call(
        kernel,
        out_shape=jax.ShapeDtypeStruct((SPAN, qw), BF16),
        in_specs=[any_space, any_space, any_space, pl.BlockSpec(memory_space=pltpu.SMEM), any_space],
        out_specs=any_space,
        scratch_shapes=[
            pltpu.VMEM((KV_HEADS, slots, wide), BF16),
            pltpu.VMEM((KV_HEADS, slots, lanes), BF16),
            pltpu.VMEM((segments.shape[0] // HEAD_DIM, HEAD_DIM), I32),
            small,
            small,
            small,
            small,
            pltpu.VMEM((Z, 8, SPAN), F32),
            small,
            pltpu.VMEM((X, 8, SPAN), F32),
            small,
            small,
            small,
            small,
            small,
            pltpu.VMEM((SPAN, 2 * SPAN), BF16),
            pltpu.VMEM((KV_HEADS, SPAN, lanes), BF16),
            pltpu.VMEM((KV_HEADS, SPAN, lanes), BF16),
            pltpu.VMEM((KV_HEADS, SPAN, wide), BF16),
            pltpu.VMEM((KV_HEADS, SPAN, wide), BF16),
            pltpu.VMEM((KV_HEADS, WINDOW, SPAN, lanes), BF16),
            pltpu.VMEM((heads, SPAN, HEAD_DIM), BF16),
            pltpu.VMEM((SPAN, WINDOW * SPAN), F32),
            pltpu.VMEM((KV_HEADS, SPAN, wide), BF16),
            pltpu.VMEM((heads, SPAN, HEAD_DIM), F32),
            pltpu.VMEM((heads, SPAN, HEAD_DIM), F32),
            pltpu.VMEM((heads, SPAN, HEAD_DIM), F32),
            pltpu.VMEM((RELAYED, (KV_HEADS - HELD) * SPAN // RELAYED, wide), BF16),
            dma((3 * KV_HEADS,)),
            dma,
            dma((KV_HEADS,)),
            dma((4,)),
            dma((4,)),
            dma((Z,)),
            dma((Z,)),
            dma((X,)),
            dma((X,)),
            dma((2 * KV_HEADS,)),
            dma((2 * KV_HEADS,)),
            dma((KV_HEADS, WINDOW)),
            dma((KV_HEADS, WINDOW)),
            dma((RELAYED,)),
            dma((RELAYED,)),
        ],
        compiler_params=pltpu.CompilerParams(
            collective_id=0, has_side_effects=True, vmem_limit_bytes=62 * 2**20
        ),
    )(query_frames, key_frames, value_frames, token_counts, segments.reshape(-1, HEAD_DIM))


def solution(mesh):
    share = P(("group", "seq"), None)
    return jax.shard_map(
        shards,
        mesh=mesh,
        in_specs=(share, share, share, P(("group", "seq")), P("group")),
        out_specs=share,
        check_vma=False,
    )
```

```python
import functools
import math

import jax
import jax.numpy as jnp
from jax import lax
from jax.experimental import pallas as pl
from jax.experimental.pallas import tpu as pltpu
from jax.sharding import PartitionSpec as P

KV_HEADS = 4
HEAD_DIM = 128
SPAN = 256
WINDOW = 5
X, Z = 4, 16
HELD = 2
RELAYED = 16
FIRST_RELAY, SECOND_RELAY = 2 * (Z - 1) // 3, (Z - 1) // 3
MESH = pl.DeviceIdType.MESH
SCALE = math.log2(math.e) / math.sqrt(HEAD_DIM)
MASKED = -1e30
BF16, F32, I32 = jnp.bfloat16, jnp.float32, jnp.int32


def kernel(
    q_hbm,
    k_hbm,
    v_hbm,
    count_ref,
    seg_hbm,
    out_hbm,
    qf,
    kvf,
    seg,
    count,
    count_prev,
    count_pair,
    pair_sum,
    column,
    column_sum,
    columns,
    base,
    base_in,
    before,
    before_in,
    lead,
    turn,
    kv_tail,
    kv_tail_in,
    q_tail,
    q_tail_in,
    kv,
    qr,
    bias,
    out,
    acc,
    top,
    total,
    relay,
    load_sem,
    seg_sem,
    out_sem,
    one_send,
    one_recv,
    z_send,
    z_recv,
    x_send,
    x_recv,
    tail_send,
    tail_recv,
    block_send,
    block_recv,
    relay_send,
    relay_recv,
):
    n = lax.axis_size("seq")
    d = lax.axis_index("seq")
    core = lax.rem(d, 2)
    chip = d // 2
    z = lax.rem(chip, Z)
    x = chip // Z
    heads = qr.shape[0] // KV_HEADS
    wide = heads * HEAD_DIM

    def at(index):
        return {"seq": lax.rem(index + n, n)}

    follower = at(d + 1)
    onward = at(d + 2)
    partner = at(d + 1 - 2 * core)

    def remote(src, dst, send, recv, device):
        return pltpu.make_async_remote_copy(
            src_ref=src,
            dst_ref=dst,
            send_sem=send,
            recv_sem=recv,
            device_id=device,
            device_id_type=MESH,
        )

    loads = []
    for g in range(KV_HEADS):
        columns_of = pl.ds(g * HEAD_DIM, HEAD_DIM)
        for part, src in enumerate((k_hbm, v_hbm)):
            loads.append(
                pltpu.make_async_copy(
                    src.at[:, columns_of],
                    kvf.at[g, :, pl.ds(part * HEAD_DIM, HEAD_DIM)],
                    load_sem.at[2 * g + part],
                )
            )
    q_loads = [
        pltpu.make_async_copy(
            q_hbm.at[:, pl.ds(g * wide, wide)],
            qf.at[g],
            load_sem.at[2 * KV_HEADS + g],
        )
        for g in range(KV_HEADS)
    ]
    seg_load = pltpu.make_async_copy(seg_hbm, seg, seg_sem)
    for load in loads + q_loads + [seg_load]:
        load.start()

    barrier = pltpu.get_barrier_semaphore()

    def greet(device):
        pl.semaphore_signal(barrier, inc=1, device_id=device, device_id_type=MESH)

    column[...] = jnp.zeros(column.shape, F32)
    columns[...] = jnp.zeros(columns.shape, F32)

    has_next, has_prev = d < n - 1, d > 0
    has_onward, has_back = d < n - 2, d > 1
    turning = x < X - 1
    source = (core == 1) & turning & (z == Z - 1)
    first_relay = (core == 1) & turning & (z == FIRST_RELAY)
    second_relay = (core == 1) & (x > 0) & (z == SECOND_RELAY)
    sink = (core == 0) & (x > 0) & (z == 0)

    def in_column(column_x, column_z, column_core):
        return at((column_x * Z + column_z) * 2 + column_core)

    pl.when(d > 0)(lambda: greet(partner))
    pl.when(has_back)(lambda: greet(at(d - 2)))
    sends_on = jnp.where(has_onward, 1, 0)
    first_chip = chip == 0
    below = (z == 0) & (x > 0)

    @pl.when(core == 0)
    def _():
        pl.when(has_prev)(lambda: greet(at(d - 1)))

        @pl.when(z > 0)
        def _():
            lax.fori_loop(z + 1, Z, lambda k, _: greet(in_column(x, k, 0)), None)

        pl.when((z > 1) | below)(lambda: greet(in_column(x, 1, 0)))

        @pl.when(z == 1)
        def _():
            pl.when(x > 0)(lambda: greet(in_column(x, 0, 0)))
            lax.fori_loop(x + 1, X, lambda k, _: greet(in_column(k, 1, 0)), None)

    pl.when(first_relay)(lambda: greet(in_column(x, Z - 1, 1)))
    pl.when(second_relay)(lambda: greet(in_column(x - 1, FIRST_RELAY, 1)))
    pl.when(sink)(lambda: greet(in_column(x, SECOND_RELAY, 1)))

    own_count = count_ref[0]
    count[...] = jnp.full(count.shape, own_count.astype(F32))

    count_copy = remote(count, count_prev, one_send.at[0], one_recv.at[0], follower)
    pair_copy = remote(count, count_pair, one_send.at[1], one_recv.at[1], partner)
    before_copy = remote(before, before_in, one_send.at[2], one_recv.at[2], partner)

    def zero(ref):
        ref[...] = jnp.zeros(ref.shape, ref.dtype)

    def start_if(there, copy):
        pl.when(there)(copy.start)

    @pl.when(core == 1)
    def _():
        also = jnp.where(source | first_relay | second_relay, 1, 0)
        beside = jnp.where(first_chip, 0, 1)
        pl.semaphore_wait(barrier, beside + jnp.where(has_next, 1, 0) + sends_on + also)
        start_if(jnp.logical_not(first_chip), pair_copy)
        start_if(has_next, count_copy)

    for load in loads:
        load.wait()

    high = own_count - SPAN
    for g in range(KV_HEADS):
        slot = lax.broadcasted_iota(I32, (SPAN, 2 * HEAD_DIM), 0)
        kv_tail[g] = jnp.where(slot < high, kvf[g, SPAN:, :], kvf[g, :SPAN, :])

    def select_q(g):
        q_loads[g].wait()
        slot = lax.broadcasted_iota(I32, (SPAN, wide), 0)
        q_tail[g] = jnp.where(slot < high, qf[g, SPAN:, :], qf[g, :SPAN, :])

    def kv_tail_copy(g):
        return remote(kv_tail.at[g], kv_tail_in.at[g], tail_send.at[g], tail_recv.at[g], follower)

    def q_tail_copy(g):
        return remote(
            q_tail.at[g],
            q_tail_in.at[g],
            tail_send.at[KV_HEADS + g],
            tail_recv.at[KV_HEADS + g],
            follower,
        )

    early = (core == 1) & (z < Z // 2)
    late = (core == 1) & (z >= Z // 2) & has_next & jnp.logical_not(source)
    piece = relay.shape[1]
    pieces = SPAN // piece

    def tail_piece(ref, j):
        return ref.at[HELD + j // pieces, pl.ds(lax.rem(j, pieces) * piece, piece)]

    def relay_in(j, device):
        return remote(tail_piece(q_tail, j), relay.at[j], relay_send.at[j], relay_recv.at[j], device)

    def relay_on(j, device):
        return remote(relay.at[j], relay.at[j], relay_send.at[j], relay_recv.at[j], device)

    def relay_out(j, device):
        arrived = tail_recv.at[KV_HEADS + HELD + j // pieces]
        return remote(relay.at[j], tail_piece(q_tail_in, j), relay_send.at[j], arrived, device)

    select_q(0)

    @pl.when(core == 1)
    def _():
        for g in range(KV_HEADS):
            start_if(has_next, kv_tail_copy(g))

    select_q(1)
    start_if((core == 1) & has_next, q_tail_copy(0))
    select_q(2)
    start_if((core == 1) & has_next, q_tail_copy(1))
    select_q(3)

    @pl.when(early)
    def _():
        for g in range(HELD, KV_HEADS):
            q_tail_copy(g).start()

    @pl.when(source)
    def _():
        to = in_column(x, FIRST_RELAY, 1)
        lax.fori_loop(0, RELAYED, lambda j, _: relay_in(j, to).start(), None)

    @pl.when(first_relay)
    def _():
        to = in_column(x + 1, SECOND_RELAY, 1)

        def pass_on(j, _):
            relay_on(j, to).wait_recv()
            relay_on(j, to).start()

        lax.fori_loop(0, RELAYED, pass_on, None)

    @pl.when(second_relay)
    def _():
        to = in_column(x, 0, 0)

        def pass_out(j, _):
            relay_on(j, to).wait_recv()
            relay_out(j, to).start()

        lax.fori_loop(0, RELAYED, pass_out, None)

    @pl.when(core == 0)
    def _():
        summing = jnp.where(z == 1, Z - 2 + jnp.minimum(x, 1) + x, jnp.maximum(z - 1, 0))
        pl.semaphore_wait(barrier, 1 + sends_on + summing + jnp.where(below, 1, 0))
        count_copy.start()

    @pl.when(d == 0)
    def _():
        count_prev[...] = jnp.full(count_prev.shape, float(SPAN), F32)
        kv_tail_in[...] = jnp.zeros(kv_tail_in.shape, BF16)
        q_tail_in[...] = jnp.zeros(q_tail_in.shape, BF16)

    @pl.when(d < 2)
    def _():
        for t in (2, 4):
            kv[:, t] = jnp.zeros((KV_HEADS, *kv.shape[2:]), BF16)

    @pl.when(core == 0)
    def _():
        @pl.when(first_chip)
        def _():
            count_pair[...] = jnp.zeros(count_pair.shape, F32)

        pl.when(jnp.logical_not(first_chip))(pair_copy.wait_recv)
        pair_sum[...] = count[...] + count_pair[...]
        column[pl.ds(z, 1)] = pair_sum[...][None]

        def pair_to(k):
            return remote(
                pair_sum, column.at[z], z_send.at[k], z_recv.at[z], in_column(x, k, 0)
            )

        def pair_from(k):
            return remote(
                pair_sum, column.at[k], z_send.at[k], z_recv.at[k], in_column(x, k, 0)
            )

        def column_to(k):
            return remote(
                column_sum, columns.at[x], x_send.at[k], x_recv.at[x], in_column(k, 1, 0)
            )

        def column_from(k):
            return remote(
                column_sum, columns.at[k], x_send.at[k], x_recv.at[k], in_column(k, 1, 0)
            )

        def base_to(k):
            return remote(base, base_in, z_send.at[k], one_recv.at[3], in_column(x, k, 0))

        base_below = remote(base_in, base_in, z_send.at[0], one_recv.at[3], in_column(x, 0, 0))

        lax.fori_loop(1, z, lambda k, _: pair_to(k).start(), None)
        pl.when(below)(lambda: pair_to(1).start())
        for g in range(KV_HEADS):
            kv_tail_copy(g).start()
            q_tail_copy(g).start()

        @pl.when(z > 0)
        def _():
            lax.fori_loop(z + 1, Z, lambda k, _: pair_from(k).wait_recv(), None)

        z_place = lax.broadcasted_iota(I32, column.shape, 0)
        x_place = lax.broadcasted_iota(I32, columns.shape, 0)
        rows = float(n * SPAN)

        @pl.when(z == 1)
        def _():
            pl.when(x > 0)(lambda: pair_from(0).wait_recv())
            column_sum[...] = jnp.sum(column[...], axis=0)
            lax.fori_loop(0, x, lambda k, _: column_to(k).start(), None)
            lax.fori_loop(x + 1, X, lambda k, _: column_from(k).wait_recv(), None)
            base[...] = jnp.sum(jnp.where(x_place > x, columns[...], 0.0), axis=0)
            base_in[...] = base[...] + column_sum[...]
            lax.fori_loop(2, Z, lambda k, _: base_to(k).start(), None)
            pl.when(x > 0)(base_below.start)
            later = jnp.sum(jnp.where(z_place >= z, column[...], 0.0), axis=0)
            before[...] = rows - (base[...] + later)

        @pl.when(z > 1)
        def _():
            base_to(z).wait_recv()
            later = jnp.sum(jnp.where(z_place >= z, column[...], 0.0), axis=0)
            before[...] = rows - (base_in[...] + later)

        @pl.when(below)
        def _():
            base_below.wait_recv()
            before[...] = rows - base_in[...]

        pl.when(first_chip)(lambda: zero(before))
        pl.when(has_prev)(count_copy.wait_recv)
        before_copy.start()
        lead[...] = before[...] - (d * SPAN).astype(F32)

        lax.fori_loop(1, z, lambda k, _: pair_to(k).wait_send(), None)
        pl.when(below)(lambda: pair_to(1).wait_send())

        @pl.when(z == 1)
        def _():
            lax.fori_loop(0, x, lambda k, _: column_to(k).wait_send(), None)
            lax.fori_loop(2, Z, lambda k, _: base_to(k).wait_send(), None)
            pl.when(x > 0)(base_below.wait_send)

        before_copy.wait_send()

    @pl.when(core == 1)
    def _():
        count_copy.wait_recv()
        before_copy.wait_recv()
        lead[...] = before_in[...] + count_prev[...] - (d * SPAN).astype(F32)
        pl.when(jnp.logical_not(first_chip))(pair_copy.wait_send)

    lead_in = lead[0:1, :].astype(I32)
    lead_before = (lead[0:1, :] - count_prev[0:1, :]).astype(I32)
    place = lax.broadcasted_iota(I32, (SPAN, SPAN), 0)
    slot = lax.broadcasted_iota(I32, (SPAN, SPAN), 1)
    step = place - slot
    arrived = (((step - lead_before) & (SPAN - 1)) == 0) & (place < lead_in)
    turn[:, :SPAN] = jnp.where(arrived, 1.0, 0.0).astype(BF16)
    turn[:, SPAN:] = jnp.where(step == lead_in, 1.0, 0.0).astype(BF16)

    def turned(tail, own):
        rows = jnp.dot(turn[:, :SPAN], tail, preferred_element_type=F32)
        rows += jnp.dot(turn[:, SPAN:], own, preferred_element_type=F32)
        return rows.astype(BF16)

    def hop(g, source, target, device):
        return remote(
            kv.at[g, source],
            kv.at[g, target],
            block_send.at[g, target],
            block_recv.at[g, target],
            device,
        )

    def arrival(g, target):
        hop(g, target, target, partner).wait_recv()

    for g in range(KV_HEADS):
        pl.when(has_prev)(kv_tail_copy(g).wait_recv)
        kv[g, 0] = turned(kv_tail_in[g], kvf[g, :SPAN, :])

    seg_load.wait()
    both = HEAD_DIM

    def clip_row(block):
        row = 2 * jnp.maximum(block, 0)
        return jnp.concatenate([seg[pl.ds(row, 1), :], seg[pl.ds(row + 1, 1), :]], axis=1).astype(F32)

    query_clip = jnp.broadcast_to(clip_row(d), (SPAN, SPAN)).T
    for t in range(WINDOW):
        same = query_clip == clip_row(d - t)
        if t == 0:
            same = same & (slot <= place)
        there = jnp.where(d >= t, 0.0, MASKED)
        bias[:, pl.ds(t * SPAN, SPAN)] = jnp.where(same, 0.0, MASKED) + there

    def send_own(g):
        start_if(has_onward, hop(g, 0, 2, onward))

        @pl.when(core == 0)
        def _():
            hop(g, 0, 1, partner).start()

    def forward(g):
        pl.when(has_back)(lambda: arrival(g, 2))
        start_if(has_onward, hop(g, 2, 4, onward))

        @pl.when(core == 0)
        def _():
            hop(g, 2, 3, partner).start()

        @pl.when(core == 1)
        def _():
            hop(g, 2, 1, partner).start()

    def forward_far(g):
        pl.when(has_back)(lambda: arrival(g, 4))

        @pl.when(core == 1)
        def _():
            hop(g, 4, 3, partner).start()

    for g in range(KV_HEADS):
        send_own(g)

    @pl.when(late)
    def _():
        for g in range(HELD, KV_HEADS):
            q_tail_copy(g).start()

    def turn_q(g):
        pl.when(has_prev)(q_tail_copy(g).wait_recv)
        rows = turned(q_tail_in[g], qf[g, :SPAN, :])
        for h in range(heads):
            qr[g * heads + h] = rows[:, h * HEAD_DIM : (h + 1) * HEAD_DIM]

    def attend(g, first, end, opening, closing):
        span = (end - first) * SPAN

        def head(h, _):
            i = g * heads + h
            keys = kv[g, first:end, :, :HEAD_DIM].reshape(span, HEAD_DIM)
            values = kv[g, first:end, :, HEAD_DIM:].reshape(span, HEAD_DIM)
            scores = lax.dot_general(
                qr[i], keys, (((1,), (1,)), ((), ())), preferred_element_type=F32
            )
            scores = scores * SCALE + bias[:, first * SPAN : end * SPAN]
            peak = jnp.max(scores, axis=1, keepdims=True)
            if not opening:
                old = top[i]
                peak = jnp.maximum(peak, old[:, :1])
            weights = jnp.exp2(scores - peak)
            sums = jnp.sum(weights, axis=1, keepdims=True)
            product = jnp.dot(weights.astype(BF16), values, preferred_element_type=F32)
            if not opening:
                factor = jnp.exp2(old - peak)
                sums = sums + total[i] * factor
                product = product + acc[i] * factor
            if closing:
                out[g, :, pl.ds(pl.multiple_of(h * HEAD_DIM, HEAD_DIM), HEAD_DIM)] = (
                    product / sums
                ).astype(BF16)
            else:
                top[i] = jnp.broadcast_to(peak, (SPAN, HEAD_DIM))
                total[i] = jnp.broadcast_to(sums, (SPAN, HEAD_DIM))
                acc[i] = product
            return 0

        lax.fori_loop(0, heads, head, 0, unroll=8)

    def out_copy(g):
        return pltpu.make_async_copy(
            out.at[g], out_hbm.at[:, pl.ds(g * wide, wide)], out_sem.at[g]
        )

    def own_step(g, _):
        turn_q(g)
        attend(g, 0, 1, True, False)

    def near_step(g, _):
        arrival(g, 1)
        attend(g, 1, 3, False, False)
        pl.when(z < Z - 1)(lambda: forward(g + HELD))

    def far_step(g, _):
        forward_far(g)
        arrival(g, 3)
        attend(g, 3, WINDOW, False, True)
        out_copy(g).start()

    def whole_step(g, _):
        turn_q(g)
        arrival(g, 1)
        arrival(g, 3)
        attend(g, 0, WINDOW, True, True)
        out_copy(g).start()

    @pl.when(z == Z - 1)
    def _():
        for g in range(KV_HEADS):
            forward(g)

    lax.fori_loop(0, HELD, own_step, None)

    @pl.when(z < Z - 1)
    def _():
        for g in range(HELD):
            forward(g)

    lax.fori_loop(0, HELD, near_step, None)
    lax.fori_loop(0, HELD, far_step, None)
    for g in range(HELD, KV_HEADS):
        forward_far(g)
    lax.fori_loop(HELD, KV_HEADS, whole_step, None)

    for g in range(KV_HEADS):
        out_copy(g).wait()
        pl.when(has_next)(kv_tail_copy(g).wait_send)
        straight = has_next if g < HELD else has_next & jnp.logical_not(source)
        pl.when(straight)(q_tail_copy(g).wait_send)
        pl.when(has_onward)(hop(g, 0, 2, onward).wait_send)
        pl.when(has_onward)(hop(g, 2, 4, onward).wait_send)
        hop(g, 2, 3, partner).wait_send()

        @pl.when(core == 0)
        def _():
            hop(g, 0, 1, partner).wait_send()

        @pl.when(core == 1)
        def _():
            hop(g, 2, 1, partner).wait_send()

    pl.when(has_next)(count_copy.wait_send)

    @pl.when(source | first_relay | second_relay)
    def _():
        lax.fori_loop(0, RELAYED, lambda j, _: relay_on(j, partner).wait_send(), None)


def shards(query_frames, key_frames, value_frames, token_counts, segments):
    slots, qw = query_frames.shape
    heads = qw // HEAD_DIM
    wide = qw // KV_HEADS
    any_space = pl.BlockSpec(memory_space=pl.ANY)
    lanes = 2 * HEAD_DIM
    small = pltpu.VMEM((8, SPAN), F32)
    dma = pltpu.SemaphoreType.DMA
    return pl.pallas_call(
        kernel,
        out_shape=jax.ShapeDtypeStruct((SPAN, qw), BF16),
        in_specs=[any_space, any_space, any_space, pl.BlockSpec(memory_space=pltpu.SMEM), any_space],
        out_specs=any_space,
        scratch_shapes=[
            pltpu.VMEM((KV_HEADS, slots, wide), BF16),
            pltpu.VMEM((KV_HEADS, slots, lanes), BF16),
            pltpu.VMEM((segments.shape[0] // HEAD_DIM, HEAD_DIM), I32),
            small,
            small,
            small,
            small,
            pltpu.VMEM((Z, 8, SPAN), F32),
            small,
            pltpu.VMEM((X, 8, SPAN), F32),
            small,
            small,
            small,
            small,
            small,
            pltpu.VMEM((SPAN, 2 * SPAN), BF16),
            pltpu.VMEM((KV_HEADS, SPAN, lanes), BF16),
            pltpu.VMEM((KV_HEADS, SPAN, lanes), BF16),
            pltpu.VMEM((KV_HEADS, SPAN, wide), BF16),
            pltpu.VMEM((KV_HEADS, SPAN, wide), BF16),
            pltpu.VMEM((KV_HEADS, WINDOW, SPAN, lanes), BF16),
            pltpu.VMEM((heads, SPAN, HEAD_DIM), BF16),
            pltpu.VMEM((SPAN, WINDOW * SPAN), F32),
            pltpu.VMEM((KV_HEADS, SPAN, wide), BF16),
            pltpu.VMEM((heads, SPAN, HEAD_DIM), F32),
            pltpu.VMEM((heads, SPAN, HEAD_DIM), F32),
            pltpu.VMEM((heads, SPAN, HEAD_DIM), F32),
            pltpu.VMEM((RELAYED, (KV_HEADS - HELD) * SPAN // RELAYED, wide), BF16),
            dma((3 * KV_HEADS,)),
            dma,
            dma((KV_HEADS,)),
            dma((4,)),
            dma((4,)),
            dma((Z,)),
            dma((Z,)),
            dma((X,)),
            dma((X,)),
            dma((2 * KV_HEADS,)),
            dma((2 * KV_HEADS,)),
            dma((KV_HEADS, WINDOW)),
            dma((KV_HEADS, WINDOW)),
            dma((RELAYED,)),
            dma((RELAYED,)),
        ],
        compiler_params=pltpu.CompilerParams(
            collective_id=0, has_side_effects=True, vmem_limit_bytes=62 * 2**20
        ),
    )(query_frames, key_frames, value_frames, token_counts, segments.reshape(-1, HEAD_DIM))


def solution(mesh):
    share = P(("group", "seq"), None)
    return jax.shard_map(
        shards,
        mesh=mesh,
        in_specs=(share, share, share, P(("group", "seq")), P("group")),
        out_specs=share,
        check_vma=False,
    )
```
